256 devices in a mesh: ctx: 32 (over y, x, core), batch: 8 (over z).
Axes of the slice: x: 4, y: 4, z: 8, core: 2. Of those that a mesh axis runs over, the one named last changes fastest.
Arguments:
- queries: bfloat16 [98304, 6144], P(('batch', 'ctx')), parts along dimension 0, may hold values from -8 to 8
- keys: bfloat16 [98304, 384], P(('batch', 'ctx')), parts along dimension 0, may hold values from -8 to 8
- values: bfloat16 [98304, 256], P(('batch', 'ctx')), parts along dimension 0, may hold values from -15 to 15
- selected: int32 [1536, 2, 16], P(('batch', 'ctx')), parts along dimension 0, may hold values from -1 to 191, as said below
Outputs:
- attended: bfloat16 [98304, 4096], P(('batch', 'ctx')), parts along dimension 0
The draws below stay inside these ranges and needn't reach their ends.
There are 8 independent parts, one for each index of `batch`. The reference program is written for one: setup_inputs(seed, part) draws one part's arguments, and reference() takes and returns one part's arrays. A program takes and returns all parts, laid end to end along the dimension named above; each array names one. Nothing has to cross between parts.
Inputs may be any that keep to these rules, and one draw needn't show every extreme that they name: `selected`: row b, group g lists distinct blocks c <= b in any order, -1 in the unused slots; blocks 0, b and b - 1 are always listed.
All inputs are finite; a program needn't handle non-finite values.
Results may differ from the reference program's by a relative error of at most 0.0048.
Values may be sent and summed in bfloat16 or wider, within the bound.
A program may use at most 128 MiB of HBM per device.

```python
import math
import jax
import jax.numpy as jnp
from jax import lax

D_HEAD = 192
D_VALUE = 128
HEADS = 32
GROUPS = 2
BLOCK = 64
SELECT = 16
TOKENS = 12288


def draw_queries(key, part):
    shape = (TOKENS, HEADS * D_HEAD)
    base_draw = jnp.clip(1.2 * jax.random.normal(jax.random.fold_in(key, 1), shape, jnp.float32), -8.0, 8.0)
    return base_draw.astype(jnp.bfloat16)


def draw_keys(key, part):
    shape = (TOKENS, GROUPS * D_HEAD)
    base_draw = jnp.clip(jax.random.normal(jax.random.fold_in(key, 2), shape, jnp.float32), -8.0, 8.0)
    return base_draw.astype(jnp.bfloat16)


def draw_selected(key, part):
    blocks = TOKENS // BLOCK
    second_key = jax.random.fold_in(key, 12)
    query_blk = jnp.arange(blocks, dtype=jnp.int32)[:, None, None]
    cand_blk = jnp.arange(blocks, dtype=jnp.int32)[None, None, :]
    causal = cand_blk <= query_blk
    candidate = cand_blk < query_blk
    must_list = causal & ((cand_blk == 0) | (cand_blk == query_blk) | (cand_blk == query_blk - 1))
    rand_part = jax.random.randint(second_key, (blocks, GROUPS, blocks), 0, 2 ** 16)
    recency = 2 ** 18 // jnp.maximum(1 + query_blk - cand_blk, 1)
    ranked = (rand_part + recency) * blocks + cand_blk
    ranked = jnp.where(must_list, 2 ** 30 + cand_blk, jnp.where(candidate, ranked, -1))
    top_vals, top_index = lax.top_k(ranked, SELECT)
    return jnp.where(top_vals >= 0, top_index, -1).astype(jnp.int32)


def level_of(own_key, extent, split, low, largest):
    def one(axis_at, blocks):
        steps = jax.random.uniform(jax.random.fold_in(jax.random.fold_in(own_key, 6), axis_at), (blocks,), jnp.float32, low / len(split), largest / len(split))
        return jnp.repeat(jnp.exp(steps), extent[axis_at] // blocks).reshape((-1,) + (1,) * (len(extent) - axis_at - 1))

    level = one(*split[0])
    for cut in split[1:]:
        level = level * one(*cut)
    return level


def noise(own_key, dims, scale, bound, pieces=(), kind=jnp.bfloat16):
    drawn = jax.random.normal(own_key, dims, jnp.float32) * scale
    if len(pieces) > 0:
        drawn = level_of(own_key, dims, pieces, -0.22, 0.18) * drawn
    return jnp.clip(drawn, min=-bound, max=bound).astype(kind)


def setup_inputs(seed: int = 0, part: int = 0) -> dict:
    key_of = jax.random.split(jax.random.key(seed), 5)
    own_keys = jax.random.split(jax.random.fold_in(key_of[4], part), 5)
    return {
        "queries": draw_queries(jax.random.fold_in(jax.random.fold_in(key_of[4], part), 71), part),
        "keys": draw_keys(jax.random.fold_in(jax.random.fold_in(key_of[4], part), 71), part),
        "values": noise(own_keys[2], (TOKENS, GROUPS * D_VALUE), 3.0, 15.0, ((0, 32),)),
        "selected": draw_selected(jax.random.fold_in(jax.random.fold_in(key_of[4], part), 71), part),
    }


def attend_exact(qblock, near_keys, near_values, chosen, block_index):
    groups, slot_count, block_len, head_dim = near_keys.shape
    value_dim = near_values.shape[3]
    key_rows = near_keys.reshape(groups, slot_count * block_len, head_dim).astype(jnp.float32)
    value_rows = near_values.reshape(groups, slot_count * block_len, value_dim).astype(jnp.float32)
    scores = jnp.einsum('qghd,gkd->gqhk', qblock.astype(jnp.float32), key_rows) * (1.0 / math.sqrt(head_dim))
    offsets = jnp.arange(block_len, dtype=jnp.int32)
    key_pos = (jnp.maximum(chosen, 0)[:, :, None] * block_len + offsets[None, None, :]).reshape(groups, -1)
    listed = jnp.broadcast_to((chosen >= 0)[:, :, None], (groups, slot_count, block_len)).reshape(groups, -1)
    query_pos = block_index * block_len + offsets
    allowed = listed[:, None, :] & (key_pos[:, None, :] <= query_pos[None, :, None])
    allowed = allowed[:, :, None, :]
    masked = jnp.where(allowed, scores, jnp.float32(-1e+30))
    row_max = lax.optimization_barrier(jnp.max(masked, axis=-1, keepdims=True))
    exp_terms = jnp.where(allowed, jnp.exp(masked - row_max), jnp.float32(0.0))
    row_sum = lax.optimization_barrier(jnp.sum(exp_terms, axis=-1, keepdims=True))
    weights = (exp_terms / row_sum).astype(jnp.bfloat16)
    result = jnp.einsum('gqhk,gkd->qghd', weights.astype(jnp.float32), value_rows)
    return result.astype(jnp.bfloat16).reshape(block_len, -1)

def reference(queries, keys, values, selected):
    blocks = TOKENS // BLOCK
    heads_per = HEADS // GROUPS
    query_blocks = queries.reshape(blocks, BLOCK, GROUPS, heads_per, D_HEAD)
    key_table = keys.reshape(blocks, BLOCK, GROUPS, D_HEAD).transpose(0, 2, 1, 3)
    value_table = values.reshape(blocks, BLOCK, GROUPS, D_VALUE).transpose(0, 2, 1, 3)
    group_ids = jnp.arange(GROUPS, dtype=jnp.int32)[:, None]

    def per_block(inputs):
        block_index, qblock, chosen = inputs
        picks = jnp.maximum(chosen, 0).astype(jnp.int32)
        return attend_exact(qblock, key_table[picks, group_ids], value_table[picks, group_ids], chosen, block_index)
    result = lax.map(per_block, (jnp.arange(blocks, dtype=jnp.int32), query_blocks, selected))
    return result.reshape(TOKENS, HEADS * D_VALUE)
```

```python
import functools
import math

import jax
import jax.numpy as jnp
from jax import lax
from jax.experimental import pallas as pl
from jax.experimental.pallas import tpu as pltpu
from jax.sharding import PartitionSpec as P

D_HEAD = 192
D_VALUE = 128
BLOCK = 64
SIDE = 4
LANES = 128
SHARD = 3
BUNDLE = SIDE * SHARD
PIECES = 24
NEG = -1e30
EMPTY = 2 * 2 * SIDE * SIDE * 3


def copies_of(first, table, send_sem, recv_sem):
    me = lax.axis_index("ctx")
    core = lax.rem(me, 2)
    chip = lax.div(me, 2)
    y = lax.div(chip, SIDE)
    x = lax.rem(chip, SIDE)
    xp, xm, x2 = (lax.rem(x + d, SIDE) for d in (1, 3, 2))
    yp, ym, y2 = (lax.rem(y + d, SIDE) for d in (1, 3, 2))

    def device(row, column):
        return (row * SIDE + column) * 2 + core

    right, left = device(y, xp), device(y, xm)
    down, up = device(yp, x), device(ym, x)
    partner = chip * 2 + (1 - core)

    def row_a(row, column):
        return (core * SIDE * SIDE + row * SIDE + column) * SHARD

    def row_b(column, row):
        return ((2 + core) * SIDE * SIDE + column * SIDE + row) * SHARD

    rest, half_bundle = SHARD - first, BUNDLE // 2
    plan = [
        (row_a(y, x), SHARD, right),
        (row_a(y, x), SHARD, left),
        (row_b(x, y), SHARD, down),
        (row_b(x, y), SHARD, up),
        (row_a(y, xm), first, right),
        (row_a(y, xp) + first, rest, left),
        (row_b(x, ym), rest, down),
        (row_b(x, yp) + rest, first, up),
        (row_a(y, 0), BUNDLE, down),
        (row_a(y, 0), BUNDLE, up),
        (row_b(x, 0), BUNDLE, right),
        (row_b(x, 0), BUNDLE, left),
        (row_a(y, 0), BUNDLE, partner),
        (row_b(x, 0), BUNDLE, partner),
        (row_a(ym, 0), half_bundle, down),
        (row_a(yp, 0) + half_bundle, half_bundle, up),
        (row_b(xm, 0), half_bundle, right),
        (row_b(xp, 0) + half_bundle, half_bundle, left),
        (row_a(ym, 0), BUNDLE, partner),
        (row_a(yp, 0), BUNDLE, partner),
        (row_b(xm, 0), BUNDLE, partner),
        (row_b(xp, 0), BUNDLE, partner),
        (row_a(y2, 0), BUNDLE, partner),
        (row_b(x2, 0), BUNDLE, partner),
    ]
    made = []
    for n, (row, count, peer) in enumerate(plan):
        place = table.at[pl.ds(row, count)]
        made.append(
            pltpu.make_async_remote_copy(
                src_ref=place,
                dst_ref=place,
                send_sem=send_sem.at[n],
                recv_sem=recv_sem.at[n],
                device_id={"ctx": peer},
                device_id_type=pl.DeviceIdType.MESH,
            )
        )
    peers = (right, left, down, up, partner)
    own = (row_a(y, x), row_b(x, y))
    return made, peers, own


def places_of(selected, first_block):
    own = first_block + lax.broadcasted_iota(jnp.int32, selected.shape, 0)
    spot = lax.broadcasted_iota(jnp.int32, selected.shape, 2)
    head = jnp.broadcast_to(selected[:, :, 0:1], selected.shape)
    listed = jnp.where(spot == 0, own, jnp.where(selected == own, head, selected))
    device = (listed * 10923) >> 16
    within = listed - 6 * device
    chip, core = device >> 1, device & 1
    turned = (chip & (SIDE - 1)) * SIDE + (chip >> 2)
    late = within >= SHARD
    place = jnp.where(late, turned, chip)
    within = jnp.where(late, within - SHARD, within)
    slot = (jnp.where(late, 2, 0) + core) * (SIDE * SIDE * SHARD) + place * SHARD + within
    used = listed >= 0
    return jnp.where(used, slot, EMPTY), jnp.where(used, 0, 1)


def kernel(
    heads_per,
    sel_ref,
    q_hbm,
    k_hbm,
    v_hbm,
    out_hbm,
    t0,
    t1,
    t2,
    t3,
    t4,
    q_stage,
    q_rows,
    weights,
    k_near,
    v_near,
    counts,
    place_stage,
    count_stage,
    place_ref,
    count_ref,
    out_stage,
    send_sem,
    recv_sem,
    load_sem,
    q_sem,
    place_sem,
    out_sem,
):
    tables = (t0, t1, t2, t3, t4)
    blocks = q_stage.shape[0]
    slots = sel_ref.shape[2]
    first_block = lax.axis_index("ctx") * blocks
    all_copies = []
    for j, table in enumerate(tables):
        made, peers, own = copies_of(1 + j % 2, table, send_sem.at[j], recv_sem.at[j])
        all_copies.append(made)

    loads = []
    for j, table in enumerate(tables):
        source = k_hbm if j < 3 else v_hbm
        column = (j if j < 3 else j - 3) * LANES
        for half in range(2):
            loads.append(
                pltpu.make_async_copy(
                    source.at[pl.ds(half * SHARD, SHARD), :, pl.ds(column, LANES)],
                    table.at[pl.ds(own[half], SHARD)],
                    load_sem.at[j * 2 + half],
                )
            )
    for load in loads:
        load.start()
    q_loads = [
        pltpu.make_async_copy(q_hbm.at[pl.ds(b * BLOCK, BLOCK)], q_stage.at[b], q_sem.at[b])
        for b in range(blocks)
    ]
    for load in q_loads:
        load.start()

    barrier = pltpu.get_barrier_semaphore()
    for peer in peers:
        pl.semaphore_signal(
            barrier, inc=1, device_id={"ctx": peer}, device_id_type=pl.DeviceIdType.MESH
        )
    pl.semaphore_wait(barrier, len(peers))

    def go(j, names):
        for n in names:
            all_copies[j][n].start()

    def arrived(j, names):
        for n in names:
            all_copies[j][n].wait_recv()

    def step1(j):
        arrived(j, range(0, 4))
        go(j, range(4, 8))

    def step2(j):
        arrived(j, range(4, 8))
        go(j, range(8, 14))

    def step3(j):
        arrived(j, range(8, 12))
        go(j, range(14, 22))

    def step4(j):
        arrived(j, range(14, 18))
        go(j, range(22, 24))

    def step5(j):
        arrived(j, (12, 13, 18, 19, 20, 21, 22, 23))
        if j < 3:
            tables[j][EMPTY] = jnp.broadcast_to(tables[j][0, 0:1, :], (BLOCK, LANES))
        else:
            tables[j][EMPTY] = jnp.zeros((BLOCK, LANES), jnp.bfloat16)

    lane = lax.broadcasted_iota(jnp.int32, (BLOCK, 2 * LANES), 1)

    def prepare(b):
        q_loads[b].wait()
        for head in range(2 * heads_per):
            group = head // heads_per
            start = head * D_HEAD
            aligned = start // LANES * LANES
            window = q_stage[b, :, aligned : aligned + 2 * LANES].astype(jnp.float32)
            shift = group * 64 - (start - aligned)
            if shift:
                window = pltpu.roll(window, shift % (2 * LANES), 1)
            keep = (lane >= 64) if group else (lane < D_HEAD)
            window = jnp.where(keep, window, 0.0).astype(jnp.bfloat16)
            at = (head - group * heads_per) * BLOCK
            q_rows[group * blocks + b, at : at + BLOCK, :] = window

    scale = math.log2(math.e) / math.sqrt(D_HEAD)
    chunk = heads_per // 2 * BLOCK
    causal = lax.broadcasted_iota(jnp.int32, (BLOCK, LANES), 1)
    causal = (causal >= BLOCK) | (causal <= lax.broadcasted_iota(jnp.int32, (BLOCK, LANES), 0))

    def score(b, group):
        low, high = tables[group], tables[group + 1]
        for i in range(slots):
            place = place_ref[b, group, i]
            at = i * BLOCK
            k_near[at : at + BLOCK, 0:LANES] = low[place]
            k_near[at : at + BLOCK, LANES : 2 * LANES] = high[place]
        pair = group * blocks + b

        def part(half, _):
            rows = pl.ds(pl.multiple_of(half * chunk, chunk), chunk)
            s = lax.dot_general(
                q_rows[pair, rows, :],
                k_near[...],
                (((1,), (1,)), ((), ())),
                preferred_element_type=jnp.float32,
            )
            edge = s[:, 0:LANES].reshape(heads_per // 2, BLOCK, LANES)
            edge = jnp.where(causal[None], edge, NEG).reshape(chunk, LANES)
            s = jnp.concatenate([edge, s[:, LANES:]], axis=1)
            top = jnp.max(s, axis=1, keepdims=True)
            weights[pair, rows, :] = jnp.exp2((s - top) * scale).astype(jnp.bfloat16)
            return 0

        lax.fori_loop(0, 2, part, 0)

    def attend(b, group):
        table = tables[3 + group]
        for i in range(slots):
            at = i * BLOCK
            v_near[at : at + BLOCK, 0:LANES] = table[place_ref[b, group, i]]
            v_near[at : at + BLOCK, LANES : 2 * LANES] = counts[count_ref[b, group, i]]
        pair = group * blocks + b
        for half in range(2):
            o = jnp.dot(
                weights[pair, half * chunk : (half + 1) * chunk, :],
                v_near[...],
                preferred_element_type=jnp.float32,
            )
            o = (o[:, 0:LANES] / o[:, LANES:]).astype(jnp.bfloat16)
            for h in range(heads_per // 2):
                column = (group * heads_per + half * (heads_per // 2) + h) * D_VALUE
                out_stage[b, :, column : column + D_VALUE] = o[h * BLOCK : (h + 1) * BLOCK]

    def score_blocks(group, low, high):
        lax.fori_loop(low, high, lambda b, c: (score(b, group), c)[1], 0)

    def attend_blocks(group, low, high):
        lax.fori_loop(low, high, lambda b, c: (attend(b, group), c)[1], 0)

    width = heads_per * D_VALUE
    stores = {}

    def put(group, b):
        columns = pl.ds(group * width, width)
        stores[group, b] = pltpu.make_async_copy(
            out_stage.at[b, :, columns],
            out_hbm.at[pl.ds(b * BLOCK, BLOCK), columns],
            out_sem.at[group * blocks + b],
        )
        stores[group, b].start()

    for j in range(5):
        loads[2 * j].wait()
        loads[2 * j + 1].wait()
        go(j, range(0, 4))
    place_stage[...], count_stage[...] = places_of(sel_ref[...], first_block)
    place_copies = [
        pltpu.make_async_copy(place_stage, place_ref, place_sem.at[0]),
        pltpu.make_async_copy(count_stage, count_ref, place_sem.at[1]),
    ]
    counts[0] = jnp.ones((BLOCK, LANES), jnp.bfloat16)
    counts[1] = jnp.zeros((BLOCK, LANES), jnp.bfloat16)
    for j in range(5):
        prepare(j)
        step1(j)
    step2(0)
    step2(1)
    for copy in place_copies:
        copy.start()
    prepare(5)
    for copy in place_copies:
        copy.wait()
    step3(0)
    step2(2)
    step3(1)
    step2(3)
    step4(0)
    step3(2)
    step2(4)
    step4(1)
    step5(0)
    step5(1)
    score_blocks(0, 0, 2)
    step3(3)
    score_blocks(0, 2, 4)
    step4(2)
    score_blocks(0, 4, 6)
    step3(4)
    step5(2)
    score_blocks(1, 0, 3)
    step4(3)
    score_blocks(1, 3, 6)
    step5(3)
    attend_blocks(0, 0, 3)
    step4(4)
    attend_blocks(0, 3, 6)
    for b in range(blocks):
        put(0, b)
    step5(4)
    attend_blocks(1, 0, 6)
    for b in range(blocks):
        put(1, b)
    for made in all_copies:
        for copy in made:
            copy.wait_send()
    for store in stores.values():
        store.wait()


def per_device(queries, keys, values, selected):
    rows = queries.shape[0]
    blocks = rows // BLOCK
    groups = keys.shape[1] // D_HEAD
    heads_per = queries.shape[1] // (groups * D_HEAD)
    entries = blocks * 2 * SIDE * SIDE + 1
    spots = selected.shape[2] * BLOCK
    anywhere = pl.BlockSpec(memory_space=pl.ANY)
    return pl.pallas_call(
        functools.partial(kernel, heads_per),
        out_shape=jax.ShapeDtypeStruct((rows, groups * heads_per * D_VALUE), jnp.bfloat16),
        in_specs=[pl.BlockSpec(memory_space=pltpu.VMEM), anywhere, anywhere, anywhere],
        out_specs=anywhere,
        scratch_shapes=[pltpu.VMEM((entries, BLOCK, LANES), jnp.bfloat16)] * 5
        + [
            pltpu.VMEM((blocks, BLOCK, queries.shape[1]), jnp.bfloat16),
            pltpu.VMEM((groups * blocks, heads_per * BLOCK, 2 * LANES), jnp.bfloat16),
            pltpu.VMEM((groups * blocks, heads_per * BLOCK, spots), jnp.bfloat16),
            pltpu.VMEM((spots, 2 * LANES), jnp.bfloat16),
            pltpu.VMEM((spots, 2 * LANES), jnp.bfloat16),
            pltpu.VMEM((2, BLOCK, LANES), jnp.bfloat16),
            pltpu.VMEM(selected.shape, jnp.int32),
            pltpu.VMEM(selected.shape, jnp.int32),
            pltpu.SMEM(selected.shape, jnp.int32),
            pltpu.SMEM(selected.shape, jnp.int32),
            pltpu.VMEM((blocks, BLOCK, groups * heads_per * D_VALUE), jnp.bfloat16),
            pltpu.SemaphoreType.DMA((5, PIECES)),
            pltpu.SemaphoreType.DMA((5, PIECES)),
            pltpu.SemaphoreType.DMA((10,)),
            pltpu.SemaphoreType.DMA((blocks,)),
            pltpu.SemaphoreType.DMA((2,)),
            pltpu.SemaphoreType.DMA((groups * blocks,)),
        ],
        compiler_params=pltpu.CompilerParams(
            collective_id=0, has_side_effects=True, vmem_limit_bytes=67043328
        ),
        name="gather_attend",
    )(
        selected,
        queries,
        keys.reshape(blocks, BLOCK, keys.shape[1]),
        values.reshape(blocks, BLOCK, values.shape[1]),
    )


def solution(mesh):
    rows = P(("batch", "ctx"), None)
    return jax.shard_map(
        per_device,
        mesh=mesh,
        in_specs=(rows, rows, rows, P(("batch", "ctx"), None, None)),
        out_specs=rows,
        check_vma=False,
    )
```

```python
import functools
import math

import jax
import jax.numpy as jnp
from jax import lax
from jax.experimental import pallas as pl
from jax.experimental.pallas import tpu as pltpu
from jax.sharding import PartitionSpec as P

D_HEAD = 192
D_VALUE = 128
BLOCK = 64
SIDE = 4
LANES = 128
SHARD = 3
BUNDLE = SIDE * SHARD
PIECES = 24
NEG = -1e30
PLAN = (
    "01", "00", "02", "q0", "03", "11", "10", "04", "12", "q1", "q2", "13", "21", "q3", "20", "q4", "q5", "22", "31",
    "30", "14", "32", "23", "41", "40", "50", "51", "s0", "42", "s1", "24", "s2", "s3", "s4", "s5", "s6", "s7", "s8",
    "33", "52", "s9", "s10", "s11", "s12", "s13", "s14", "s15", "s16", "34", "s17", "s18", "s19", "s20",
    "43", "s21", "s22", "s23", "s24", "53", "v0", "v1", "44", "v2", "v3", "v4", "v5", "54", "v6", "v7", "v8", "v9",
    "v10", "v11",
)
SENT = ("v0", "v1", "v2", "v3", "v10")
EMPTY = 2 * 2 * SIDE * SIDE * 3


def peers_and_rows():
    me = lax.axis_index("ctx")
    core = lax.rem(me, 2)
    chip = lax.div(me, 2)
    y = lax.div(chip, SIDE)
    x = lax.rem(chip, SIDE)
    xp, xm, x2 = (lax.rem(x + d, SIDE) for d in (1, 3, 2))
    yp, ym, y2 = (lax.rem(y + d, SIDE) for d in (1, 3, 2))
    parts = lax.axis_size("batch")
    part = lax.axis_index("batch")

    def device(row, column, on_chip):
        return ((row * SIDE + column) * 2 + on_chip) * parts + part

    def bundle(half, line):
        return ((half * 2 + core) * SIDE + line) * BUNDLE

    peers = dict(
        right=device(y, xp, core),
        left=device(y, xm, core),
        down=device(yp, x, core),
        up=device(ym, x, core),
        partner=device(y, x, 1 - core),
    )
    row = bundle(0, y)
    column = bundle(1, x)
    rows = dict(
        row=row,
        row_own=row + x * SHARD,
        row_left=row + xm * SHARD,
        row_right=row + xp * SHARD,
        row_up=bundle(0, ym),
        row_down=bundle(0, yp),
        row_far=bundle(0, y2),
        column=column,
        column_own=column + y * SHARD,
        column_up=column + ym * SHARD,
        column_down=column + yp * SHARD,
        column_left=bundle(1, xm),
        column_right=bundle(1, xp),
        column_far=bundle(1, x2),
    )
    return peers, rows


def copies_of(first, peers, rows, table, send_sem, recv_sem):
    rest, half = SHARD - first, BUNDLE // 2
    plan = [
        ("row_own", 0, SHARD, "right"),
        ("row_own", 0, SHARD, "left"),
        ("column_own", 0, SHARD, "down"),
        ("column_own", 0, SHARD, "up"),
        ("row_left", 0, first, "right"),
        ("row_right", first, rest, "left"),
        ("column_up", 0, rest, "down"),
        ("column_down", rest, first, "up"),
        ("row", 0, BUNDLE, "down"),
        ("row", 0, BUNDLE, "up"),
        ("column", 0, BUNDLE, "right"),
        ("column", 0, BUNDLE, "left"),
        ("row", 0, BUNDLE, "partner"),
        ("column", 0, BUNDLE, "partner"),
        ("row_up", 0, half, "down"),
        ("row_down", half, half, "up"),
        ("column_left", 0, half, "right"),
        ("column_right", half, half, "left"),
        ("row_up", 0, BUNDLE, "partner"),
        ("row_down", 0, BUNDLE, "partner"),
        ("column_left", 0, BUNDLE, "partner"),
        ("column_right", 0, BUNDLE, "partner"),
        ("row_far", 0, BUNDLE, "partner"),
        ("column_far", 0, BUNDLE, "partner"),
    ]
    made = []
    for n, (name, skip, count, peer) in enumerate(plan):
        place = table.at[pl.ds(rows[name] + skip, count)]
        made.append(
            pltpu.make_async_remote_copy(
                src_ref=place,
                dst_ref=place,
                send_sem=send_sem.at[n],
                recv_sem=recv_sem.at[n],
                device_id=peers[peer],
                device_id_type=pl.DeviceIdType.LOGICAL,
            )
        )
    return made


def places_of(selected, first_block):
    own = first_block + lax.broadcasted_iota(jnp.int32, selected.shape, 0)
    spot = lax.broadcasted_iota(jnp.int32, selected.shape, 2)
    head = jnp.broadcast_to(selected[:, :, 0:1], selected.shape)
    listed = jnp.where(spot == 0, own, jnp.where(selected == own, head, selected))
    device = (listed * 10923) >> 16
    within = listed - 6 * device
    chip, core = device >> 1, device & 1
    turned = (chip & (SIDE - 1)) * SIDE + (chip >> 2)
    late = within >= SHARD
    place = jnp.where(late, turned, chip)
    within = jnp.where(late, within - SHARD, within)
    slot = (jnp.where(late, 2, 0) + core) * (SIDE * SIDE * SHARD) + place * SHARD + within
    used = listed >= 0
    return jnp.where(used, slot, EMPTY), jnp.where(used, 0, 1)


def kernel(
    heads_per,
    sel_ref,
    q_hbm,
    k_hbm,
    v_hbm,
    out_ref,
    t0,
    t1,
    t2,
    t3,
    t4,
    scores_a,
    scores_b,
    weights,
    near_rows,
    counts,
    sel_stage,
    place_stage,
    count_stage,
    place_ref,
    count_ref,
    send_sem,
    recv_sem,
    load_sem,
    q_sem,
    place_sem,
):
    tables = (t0, t1, t2, t3, t4)
    scores = (scores_a, scores_b)
    blocks, groups, slots = sel_ref.shape
    first_block = lax.axis_index("ctx") * blocks
    peers, rows = peers_and_rows()
    barrier = pltpu.get_barrier_semaphore()
    for peer in peers.values():
        pl.semaphore_signal(
            barrier, inc=1, device_id=peer, device_id_type=pl.DeviceIdType.LOGICAL
        )

    own = (rows["row_own"], rows["column_own"])
    loads = []
    for j, table in enumerate(tables):
        source = k_hbm if j < 3 else v_hbm
        column = (j if j < 3 else j - 3) * LANES
        for half in range(2):
            loads.append(
                pltpu.make_async_copy(
                    source.at[pl.ds(half * SHARD, SHARD), :, pl.ds(column, LANES)],
                    table.at[pl.ds(own[half], SHARD)],
                    load_sem.at[j * 2 + half],
                )
            )
    for load in loads:
        load.start()
    near = 2 * LANES
    strips = 2 * heads_per // 4
    q_loads = [
        [
            pltpu.make_async_copy(
                q_hbm.at[pl.ds(b * BLOCK, BLOCK), pl.ds(i * 4 * D_HEAD, 4 * D_HEAD)],
                weights.at[
                    (groups - 1) * blocks + b,
                    pl.ds(i * BLOCK, BLOCK),
                    pl.ds(near, 4 * D_HEAD),
                ],
                q_sem.at[b, i],
            )
            for i in range(strips)
        ]
        for b in range(blocks)
    ]
    for group in q_loads:
        for load in group:
            load.start()

    sel_load = pltpu.make_async_copy(sel_ref, sel_stage, place_sem.at[2])
    sel_load.start()
    pl.semaphore_wait(barrier, len(peers))

    all_copies = {}

    def go(j, names):
        for n in names:
            all_copies[j][n].start()

    def arrived(j, names):
        for n in names:
            all_copies[j][n].wait_recv()

    def step1(j):
        arrived(j, range(0, 4))
        go(j, range(4, 8))

    def step2(j):
        arrived(j, range(4, 8))
        go(j, range(8, 14))

    def step3(j):
        arrived(j, range(8, 12))
        go(j, range(14, 22))

    def step4(j):
        arrived(j, range(14, 18))
        go(j, range(22, 24))

    def step5(j):
        arrived(j, (12, 13, 18, 19, 20, 21, 22, 23))
        if j < 3:
            tables[j][EMPTY] = jnp.broadcast_to(tables[j][0, 0:1, :], (BLOCK, LANES))
        else:
            tables[j][EMPTY] = jnp.zeros((BLOCK, LANES), jnp.bfloat16)

    lane = lax.broadcasted_iota(jnp.int32, (BLOCK, 2 * LANES), 1)

    def prepare(b):
        for load in q_loads[b]:
            load.wait()
        for head in range(2 * heads_per):
            group = head // heads_per
            start = head % 4 * D_HEAD
            aligned = start // LANES * LANES
            strip = head // 4 * BLOCK
            window = weights[
                (groups - 1) * blocks + b,
                strip : strip + BLOCK,
                near + aligned : near + aligned + near,
            ].astype(jnp.float32)
            shift = group * 64 - (start - aligned)
            if shift:
                window = pltpu.roll(window, shift % (2 * LANES), 1)
            keep = (lane >= 64) if group else (lane < D_HEAD)
            window = jnp.where(keep, window, 0.0).astype(jnp.bfloat16)
            at = (head - group * heads_per) * BLOCK
            weights[group * blocks + b, at : at + BLOCK, 0:near] = window

    scale = math.log2(math.e) / math.sqrt(D_HEAD)
    chunk = heads_per // 2 * BLOCK
    causal = lax.broadcasted_iota(jnp.int32, (BLOCK, LANES), 1)
    causal = (causal >= BLOCK) | (causal <= lax.broadcasted_iota(jnp.int32, (BLOCK, LANES), 0))

    half_heads = heads_per // 2

    def near_keys(pair):
        group, b = divmod(pair, blocks)
        low, high = tables[group], tables[group + 1]
        for i in range(slots):
            place = place_ref[b, group, i]
            at = i * BLOCK
            near_rows[pair % 2, at : at + BLOCK, 0:LANES] = low[place]
            near_rows[pair % 2, at : at + BLOCK, LANES : 2 * LANES] = high[place]

    def near_values(pair):
        group, b = divmod(pair, blocks)
        table = tables[3 + group]
        for i in range(slots):
            at = i * BLOCK
            near_rows[pair % 2, at : at + BLOCK, 0:LANES] = table[place_ref[b, group, i]]
            near_rows[pair % 2, at : at + BLOCK, LANES : 2 * LANES] = counts[count_ref[b, group, i]]

    def multiply(unit):
        pair, half = divmod(unit, 2)
        scores[half][...] = lax.dot_general(
            weights[pair, half * chunk : (half + 1) * chunk, 0:near],
            near_rows[pair % 2],
            (((1,), (1,)), ((), ())),
            preferred_element_type=jnp.float32,
        )

    def soften(unit):
        pair, half = divmod(unit, 2)
        s = scores[half][...]
        edge = s[:, 0:LANES].reshape(half_heads, BLOCK, LANES)
        edge = jnp.where(causal[None], edge, NEG).reshape(chunk, LANES)
        s = jnp.concatenate([edge, s[:, LANES:]], axis=1)
        top = jnp.max(s, axis=1, keepdims=True)
        weights[pair, half * chunk : (half + 1) * chunk, :] = jnp.exp2((s - top) * scale).astype(
            jnp.bfloat16
        )

    units = groups * blocks * 2

    def stage(n):
        if n % (2 * blocks) == 0 and n < units:
            near_keys(n // 2)
        if n < units:
            multiply(n)
        if n > 0:
            soften(n - 1)
        if n % 2 and (n + 1) % (2 * blocks):
            near_keys((n + 1) // 2)

    def attend(pair):
        group, b = divmod(pair, blocks)
        if b == 0:
            near_values(pair)
        if b + 1 < blocks:
            near_values(pair + 1)
        for half in range(2):
            o = jnp.dot(
                weights[pair, half * chunk : (half + 1) * chunk, :],
                near_rows[pair % 2],
                preferred_element_type=jnp.float32,
            )
            o = (o[:, 0:LANES] / o[:, LANES:]).astype(jnp.bfloat16)
            for h in range(half_heads):
                column = (group * heads_per + half * half_heads + h) * D_VALUE
                out_ref[b * BLOCK : (b + 1) * BLOCK, column : column + D_VALUE] = o[
                    h * BLOCK : (h + 1) * BLOCK
                ]

    def send_own(j):
        all_copies[j] = copies_of(
            1 + j % 2, peers, rows, tables[j], send_sem.at[j], recv_sem.at[j]
        )
        loads[2 * j].wait()
        loads[2 * j + 1].wait()
        go(j, range(0, 4))

    counts[0] = jnp.ones((BLOCK, LANES), jnp.bfloat16)
    counts[1] = jnp.zeros((BLOCK, LANES), jnp.bfloat16)
    place_copies = [
        pltpu.make_async_copy(place_stage, place_ref, place_sem.at[0]),
        pltpu.make_async_copy(count_stage, count_ref, place_sem.at[1]),
    ]
    steps = {
        "0": send_own,
        "1": step1,
        "2": step2,
        "3": step3,
        "4": step4,
        "5": step5,
        "q": prepare,
        "s": stage,
        "v": attend,
    }
    for step in PLAN:
        if step == "s0":
            for copy in place_copies:
                copy.wait()
        steps[step[0]](int(step[1:]))
        if step in SENT:
            for copy in all_copies[SENT.index(step)]:
                copy.wait_send()
        if step == "q0":
            sel_load.wait()
            place_stage[...], count_stage[...] = places_of(sel_stage[...], first_block)
        if step == "q1":
            for copy in place_copies:
                copy.start()


def per_device(queries, keys, values, selected):
    rows = queries.shape[0]
    blocks = rows // BLOCK
    groups = keys.shape[1] // D_HEAD
    heads_per = queries.shape[1] // (groups * D_HEAD)
    entries = blocks * 2 * SIDE * SIDE + 1
    spots = selected.shape[2] * BLOCK
    anywhere = pl.BlockSpec(memory_space=pl.ANY)
    return pl.pallas_call(
        functools.partial(kernel, heads_per),
        out_shape=pltpu.VMEM((rows, groups * heads_per * D_VALUE), jnp.bfloat16),
        in_specs=[anywhere, anywhere, anywhere, anywhere],
        out_specs=pl.BlockSpec(memory_space=pltpu.VMEM),
        scratch_shapes=[pltpu.VMEM((entries, BLOCK, LANES), jnp.bfloat16)] * 5
        + [pltpu.VMEM((heads_per // 2 * BLOCK, spots), jnp.float32)] * 2
        + [
            pltpu.VMEM((groups * blocks, heads_per * BLOCK, spots), jnp.bfloat16),
            pltpu.VMEM((2, spots, 2 * LANES), jnp.bfloat16),
            pltpu.VMEM((2, BLOCK, LANES), jnp.bfloat16),
            pltpu.VMEM(selected.shape, jnp.int32),
            pltpu.VMEM(selected.shape, jnp.int32),
            pltpu.VMEM(selected.shape, jnp.int32),
            pltpu.SMEM(selected.shape, jnp.int32),
            pltpu.SMEM(selected.shape, jnp.int32),
            pltpu.SemaphoreType.DMA((5, PIECES)),
            pltpu.SemaphoreType.DMA((5, PIECES)),
            pltpu.SemaphoreType.DMA((10,)),
            pltpu.SemaphoreType.DMA((blocks, groups * heads_per // 4)),
            pltpu.SemaphoreType.DMA((3,)),
        ],
        compiler_params=pltpu.CompilerParams(
            collective_id=0, has_side_effects=True, vmem_limit_bytes=60 * 1000 * 1000
        ),
        name="gather_attend",
    )(
        selected,
        queries,
        keys.reshape(blocks, BLOCK, keys.shape[1]),
        values.reshape(blocks, BLOCK, values.shape[1]),
    )


def solution(mesh):
    rows = P(("batch", "ctx"), None)
    return jax.shard_map(
        per_device,
        mesh=mesh,
        in_specs=(rows, rows, rows, P(("batch", "ctx"), None, None)),
        out_specs=rows,
        check_vma=False,
    )
```

```python
import functools
import math

import jax
import jax.numpy as jnp
from jax import lax
from jax.experimental import pallas as pl
from jax.experimental.pallas import tpu as pltpu
from jax.sharding import PartitionSpec as P

D_HEAD = 192
D_VALUE = 128
BLOCK = 64
SIDE = 4
LANES = 128
SHARD = 3
BUNDLE = SIDE * SHARD
PIECES = 28
NEG = -1e30
PLAN = (
    "01", "q0", "q1", "00", "02", "03", "11", "04", "10", "12", "13", "21", "71", "q2",
    "20", "70", "q3", "q4", "31", "30", "22", "72", "q5", "41", "60", "14", "61", "40",
    "32", "23", "73", "50", "51", "s0", "s1", "s2", "62", "s3", "s4", "s5", "s6", "24",
    "42", "s7", "s8", "s9", "s10", "33", "74", "s11", "52", "s12", "s13", "s14", "s15", "s16",
    "34", "63", "s17", "s18", "s19", "s20", "43", "s21", "s22", "s23", "64", "s24", "53", "v0",
    "v1", "v2", "44", "v3", "v4", "v5", "54", "v6", "v7", "v8", "v9", "v10", "v11",
)
SENT = ("s6", "s10", "s16", "s24", "v10")
EMPTY = 2 * 2 * SIDE * SIDE * 3


def peers_and_rows():
    me = lax.axis_index("ctx")
    core = lax.rem(me, 2)
    chip = lax.div(me, 2)
    y = lax.div(chip, SIDE)
    x = lax.rem(chip, SIDE)
    xp, xm, x2 = (lax.rem(x + d, SIDE) for d in (1, 3, 2))
    yp, ym, y2 = (lax.rem(y + d, SIDE) for d in (1, 3, 2))
    parts = lax.axis_size("batch")
    part = lax.axis_index("batch")

    def device(row, column, on_chip):
        return ((row * SIDE + column) * 2 + on_chip) * parts + part

    def bundle(half, line):
        return ((half * 2 + core) * SIDE + line) * BUNDLE

    peers = dict(
        right=device(y, xp, core),
        left=device(y, xm, core),
        down=device(yp, x, core),
        up=device(ym, x, core),
        partner=device(y, x, 1 - core),
    )
    row = bundle(0, y)
    column = bundle(1, x)
    rows = dict(
        row=row,
        row_own=row + x * SHARD,
        row_left=row + xm * SHARD,
        row_right=row + xp * SHARD,
        row_up=bundle(0, ym),
        row_down=bundle(0, yp),
        row_far=bundle(0, y2),
        column=column,
        column_own=column + y * SHARD,
        column_up=column + ym * SHARD,
        column_down=column + yp * SHARD,
        column_left=bundle(1, xm),
        column_right=bundle(1, xp),
        column_far=bundle(1, x2),
    )
    return peers, rows


def copies_of(first, peers, rows, table, send_sem, recv_sem):
    rest, half = SHARD - first, BUNDLE // 2
    plan = [
        ("row_own", 0, SHARD, "right"),
        ("row_own", 0, SHARD, "left"),
        ("column_own", 0, SHARD, "down"),
        ("column_own", 0, SHARD, "up"),
        ("row_left", 0, first, "right"),
        ("row_right", first, rest, "left"),
        ("column_up", 0, rest, "down"),
        ("column_down", rest, first, "up"),
        ("row", 0, half, "down"),
        ("row", half, half, "up"),
        ("column", 0, half, "right"),
        ("column", half, half, "left"),
        ("row", 0, BUNDLE, "partner"),
        ("column", 0, BUNDLE, "partner"),
        ("row_up", 0, half, "down"),
        ("row_down", half, half, "up"),
        ("column_left", 0, half, "right"),
        ("column_right", half, half, "left"),
        ("row_up", 0, BUNDLE, "partner"),
        ("row_down", 0, BUNDLE, "partner"),
        ("column_left", 0, BUNDLE, "partner"),
        ("column_right", 0, BUNDLE, "partner"),
        ("row_far", 0, BUNDLE, "partner"),
        ("column_far", 0, BUNDLE, "partner"),
        ("row", half, half, "down"),
        ("row", 0, half, "up"),
        ("column", half, half, "right"),
        ("column", 0, half, "left"),
    ]
    made = []
    for n, (name, skip, count, peer) in enumerate(plan):
        place = table.at[pl.ds(rows[name] + skip, count)]
        made.append(
            pltpu.make_async_remote_copy(
                src_ref=place,
                dst_ref=place,
                send_sem=send_sem.at[n],
                recv_sem=recv_sem.at[n],
                device_id=peers[peer],
                device_id_type=pl.DeviceIdType.LOGICAL,
            )
        )
    return made


def places_of(selected, first_block):
    own = first_block + lax.broadcasted_iota(jnp.int32, selected.shape, 0)
    spot = lax.broadcasted_iota(jnp.int32, selected.shape, 2)
    head = jnp.broadcast_to(selected[:, :, 0:1], selected.shape)
    listed = jnp.where(spot == 0, own, jnp.where(selected == own, head, selected))
    device = (listed * 10923) >> 16
    within = listed - 6 * device
    chip, core = device >> 1, device & 1
    turned = (chip & (SIDE - 1)) * SIDE + (chip >> 2)
    late = within >= SHARD
    place = jnp.where(late, turned, chip)
    within = jnp.where(late, within - SHARD, within)
    slot = (jnp.where(late, 2, 0) + core) * (SIDE * SIDE * SHARD) + place * SHARD + within
    used = listed >= 0
    return jnp.where(used, slot, EMPTY), jnp.where(used, 0, 1)


def kernel(
    heads_per,
    sel_ref,
    q_hbm,
    k_hbm,
    v_hbm,
    out_ref,
    t0,
    t1,
    t2,
    t3,
    t4,
    scores_a,
    scores_b,
    weights,
    near_rows,
    counts,
    sel_stage,
    place_stage,
    count_stage,
    place_ref,
    count_ref,
    send_sem,
    recv_sem,
    load_sem,
    q_sem,
    place_sem,
):
    tables = (t0, t1, t2, t3, t4)
    scores = (scores_a, scores_b)
    blocks, groups, slots = sel_ref.shape
    first_block = lax.axis_index("ctx") * blocks
    peers, rows = peers_and_rows()
    barrier = pltpu.get_barrier_semaphore()
    for peer in peers.values():
        pl.semaphore_signal(
            barrier, inc=1, device_id=peer, device_id_type=pl.DeviceIdType.LOGICAL
        )

    own = (rows["row_own"], rows["column_own"])
    loads = []
    for j, table in enumerate(tables):
        source = k_hbm if j < 3 else v_hbm
        column = (j if j < 3 else j - 3) * LANES
        for half in range(2):
            loads.append(
                pltpu.make_async_copy(
                    source.at[pl.ds(half * SHARD, SHARD), :, pl.ds(column, LANES)],
                    table.at[pl.ds(own[half], SHARD)],
                    load_sem.at[j * 2 + half],
                )
            )
    for load in loads:
        load.start()
    near = 2 * LANES
    strips = 2 * heads_per // 4
    q_loads = [
        [
            pltpu.make_async_copy(
                q_hbm.at[pl.ds(b * BLOCK, BLOCK), pl.ds(i * 4 * D_HEAD, 4 * D_HEAD)],
                weights.at[
                    (groups - 1) * blocks + b,
                    pl.ds(i * BLOCK, BLOCK),
                    pl.ds(near, 4 * D_HEAD),
                ],
                q_sem.at[b, i],
            )
            for i in range(strips)
        ]
        for b in range(blocks)
    ]
    for group in q_loads:
        for load in group:
            load.start()

    sel_load = pltpu.make_async_copy(sel_ref, sel_stage, place_sem.at[2])
    sel_load.start()
    pl.semaphore_wait(barrier, len(peers))

    all_copies = {}

    def go(j, names):
        for n in names:
            all_copies[j][n].start()

    def arrived(j, names):
        for n in names:
            all_copies[j][n].wait_recv()

    def step1(j):
        arrived(j, range(0, 4))
        go(j, range(4, 8))

    def step2(j):
        arrived(j, range(4, 8))
        go(j, range(8, 14))

    def step7(j):
        go(j, range(24, 28))

    def step3(j):
        arrived(j, range(8, 12))
        go(j, range(14, 18))

    def step6(j):
        arrived(j, range(24, 28))
        go(j, range(18, 22))

    def step4(j):
        arrived(j, range(14, 18))
        go(j, range(22, 24))

    def step5(j):
        arrived(j, (12, 13, 18, 19, 20, 21, 22, 23))
        if j < 3:
            tables[j][EMPTY] = jnp.broadcast_to(tables[j][0, 0:1, :], (BLOCK, LANES))
        else:
            tables[j][EMPTY] = jnp.zeros((BLOCK, LANES), jnp.bfloat16)

    lane = lax.broadcasted_iota(jnp.int32, (BLOCK, 2 * LANES), 1)

    def prepare(b):
        for load in q_loads[b]:
            load.wait()
        for head in range(2 * heads_per):
            group = head // heads_per
            start = head % 4 * D_HEAD
            aligned = start // LANES * LANES
            strip = head // 4 * BLOCK
            window = weights[
                (groups - 1) * blocks + b,
                strip : strip + BLOCK,
                near + aligned : near + aligned + near,
            ].astype(jnp.float32)
            shift = group * 64 - (start - aligned)
            if shift:
                window = pltpu.roll(window, shift % (2 * LANES), 1)
            keep = (lane >= 64) if group else (lane < D_HEAD)
            window = jnp.where(keep, window, 0.0).astype(jnp.bfloat16)
            at = (head - group * heads_per) * BLOCK
            weights[group * blocks + b, at : at + BLOCK, 0:near] = window

    scale = math.log2(math.e) / math.sqrt(D_HEAD)
    chunk = heads_per // 2 * BLOCK
    causal = lax.broadcasted_iota(jnp.int32, (BLOCK, LANES), 1)
    causal = (causal >= BLOCK) | (causal <= lax.broadcasted_iota(jnp.int32, (BLOCK, LANES), 0))

    half_heads = heads_per // 2

    def near_keys(pair):
        group, b = divmod(pair, blocks)
        low, high = tables[group], tables[group + 1]
        for i in range(slots):
            place = place_ref[b, group, i]
            at = i * BLOCK
            near_rows[pair % 2, at : at + BLOCK, 0:LANES] = low[place]
            near_rows[pair % 2, at : at + BLOCK, LANES : 2 * LANES] = high[place]

    def near_values(pair):
        group, b = divmod(pair, blocks)
        table = tables[3 + group]
        for i in range(slots):
            at = i * BLOCK
            near_rows[pair % 2, at : at + BLOCK, 0:LANES] = table[place_ref[b, group, i]]
            near_rows[pair % 2, at : at + BLOCK, LANES : 2 * LANES] = counts[count_ref[b, group, i]]

    def multiply(unit):
        pair, half = divmod(unit, 2)
        scores[half][...] = lax.dot_general(
            weights[pair, half * chunk : (half + 1) * chunk, 0:near],
            near_rows[pair % 2],
            (((1,), (1,)), ((), ())),
            preferred_element_type=jnp.float32,
        )

    def soften(unit):
        pair, half = divmod(unit, 2)
        s = scores[half][...]
        edge = s[:, 0:LANES].reshape(half_heads, BLOCK, LANES)
        edge = jnp.where(causal[None], edge, NEG).reshape(chunk, LANES)
        s = jnp.concatenate([edge, s[:, LANES:]], axis=1)
        top = jnp.max(s, axis=1, keepdims=True)
        weights[pair, half * chunk : (half + 1) * chunk, :] = jnp.exp2((s - top) * scale).astype(
            jnp.bfloat16
        )

    units = groups * blocks * 2

    def stage(n):
        if n % (2 * blocks) == 0 and n < units:
            near_keys(n // 2)
        if n < units:
            multiply(n)
        if n > 0:
            soften(n - 1)
        if n % 2 and (n + 1) % (2 * blocks):
            near_keys((n + 1) // 2)

    def attend(pair):
        group, b = divmod(pair, blocks)
        if b == 0:
            near_values(pair)
        if b + 1 < blocks:
            near_values(pair + 1)
        for half in range(2):
            o = jnp.dot(
                weights[pair, half * chunk : (half + 1) * chunk, :],
                near_rows[pair % 2],
                preferred_element_type=jnp.float32,
            )
            o = (o[:, 0:LANES] / o[:, LANES:]).astype(jnp.bfloat16)
            for h in range(half_heads):
                column = (group * heads_per + half * half_heads + h) * D_VALUE
                out_ref[b * BLOCK : (b + 1) * BLOCK, column : column + D_VALUE] = o[
                    h * BLOCK : (h + 1) * BLOCK
                ]

    def send_own(j):
        all_copies[j] = copies_of(
            1 + j % 2, peers, rows, tables[j], send_sem.at[j], recv_sem.at[j]
        )
        loads[2 * j].wait()
        loads[2 * j + 1].wait()
        go(j, range(0, 4))

    counts[0] = jnp.ones((BLOCK, LANES), jnp.bfloat16)
    counts[1] = jnp.zeros((BLOCK, LANES), jnp.bfloat16)
    place_copies = [
        pltpu.make_async_copy(place_stage, place_ref, place_sem.at[0]),
        pltpu.make_async_copy(count_stage, count_ref, place_sem.at[1]),
    ]
    steps = {
        "0": send_own,
        "1": step1,
        "2": step2,
        "3": step3,
        "4": step4,
        "5": step5,
        "6": step6,
        "7": step7,
        "q": prepare,
        "s": stage,
        "v": attend,
    }
    for step in PLAN:
        if step == "s0":
            for copy in place_copies:
                copy.wait()
        steps[step[0]](int(step[1:]))
        if step in SENT:
            for copy in all_copies[SENT.index(step)]:
                copy.wait_send()
        if step == "q0":
            sel_load.wait()
            place_stage[...], count_stage[...] = places_of(sel_stage[...], first_block)
        if step == "q1":
            for copy in place_copies:
                copy.start()


def per_device(queries, keys, values, selected):
    rows = queries.shape[0]
    blocks = rows // BLOCK
    groups = keys.shape[1] // D_HEAD
    heads_per = queries.shape[1] // (groups * D_HEAD)
    entries = blocks * 2 * SIDE * SIDE + 1
    spots = selected.shape[2] * BLOCK
    anywhere = pl.BlockSpec(memory_space=pl.ANY)
    return pl.pallas_call(
        functools.partial(kernel, heads_per),
        out_shape=pltpu.VMEM((rows, groups * heads_per * D_VALUE), jnp.bfloat16),
        in_specs=[anywhere, anywhere, anywhere, anywhere],
        out_specs=pl.BlockSpec(memory_space=pltpu.VMEM),
        scratch_shapes=[pltpu.VMEM((entries, BLOCK, LANES), jnp.bfloat16)] * 5
        + [pltpu.VMEM((heads_per // 2 * BLOCK, spots), jnp.float32)] * 2
        + [
            pltpu.VMEM((groups * blocks, heads_per * BLOCK, spots), jnp.bfloat16),
            pltpu.VMEM((2, spots, 2 * LANES), jnp.bfloat16),
            pltpu.VMEM((2, BLOCK, LANES), jnp.bfloat16),
            pltpu.VMEM(selected.shape, jnp.int32),
            pltpu.VMEM(selected.shape, jnp.int32),
            pltpu.VMEM(selected.shape, jnp.int32),
            pltpu.SMEM(selected.shape, jnp.int32),
            pltpu.SMEM(selected.shape, jnp.int32),
            pltpu.SemaphoreType.DMA((5, PIECES)),
            pltpu.SemaphoreType.DMA((5, PIECES)),
            pltpu.SemaphoreType.DMA((10,)),
            pltpu.SemaphoreType.DMA((blocks, groups * heads_per // 4)),
            pltpu.SemaphoreType.DMA((3,)),
        ],
        compiler_params=pltpu.CompilerParams(
            collective_id=0, has_side_effects=True, vmem_limit_bytes=60 * 1000 * 1000
        ),
        name="gather_attend",
    )(
        selected,
        queries,
        keys.reshape(blocks, BLOCK, keys.shape[1]),
        values.reshape(blocks, BLOCK, values.shape[1]),
    )


def solution(mesh):
    rows = P(("batch", "ctx"), None)
    return jax.shard_map(
        per_device,
        mesh=mesh,
        in_specs=(rows, rows, rows, P(("batch", "ctx"), None, None)),
        out_specs=rows,
        check_vma=False,
    )
```
